32 devices in a mesh: gx: 4 (over y, x), gy: 2 (over core), gz: 4 (over z).
Axes of the slice: x: 2, y: 2, z: 4, core: 2. Of those that a mesh axis runs over, the one named last changes fastest.
Arguments:
- labels: int32 [128, 128, 512], P('gx', 'gy', 'gz'), may hold values from 0 to 7
- conductivity: float32 [7, 8], replicated, may hold values from -0.08 to 2, as said below
- right_side: float32 [128, 128, 512], P('gx', 'gy', 'gz'), may hold values from -18 to 18
Outputs:
- solution: float32 [128, 128, 512], P('gx', 'gy', 'gz')
The draws below stay inside these ranges and needn't reach their ends.
Inputs may be any that keep to these rules, and one draw needn't show every extreme that they name: `conductivity`: rows 0 to 2 are positive, rows 3 to 5 have magnitude at most 0.08, row 6 is at least 0.5.
All inputs are finite; a program needn't handle non-finite values.
Results may differ from the reference program's by a relative error of at most 0.0001.
Values sent between devices are 32-bit elements; how exact they have to be, the bound alone decides.
A program may use at most 128 MiB of HBM per device.

```python
import math
import jax
import jax.numpy as jnp
from jax import lax

ITERS = 3
LABELS = 8
NX = 128
NY = 128
NZ = 512


def draw_conductivity(key, part):
    key_diag = jax.random.fold_in(key, 11)
    key_off = jax.random.fold_in(key, 12)
    key_mass = jax.random.fold_in(key, 13)
    diagonal = jnp.exp(jax.random.uniform(key_diag, (3, LABELS), jnp.float32, math.log(0.5), math.log(2.0)))
    offdiag = jax.random.uniform(key_off, (3, LABELS), jnp.float32, -0.08, 0.08)
    mass = jnp.exp(jax.random.uniform(key_mass, (1, LABELS), jnp.float32, math.log(0.5), math.log(1.0)))
    return jnp.concatenate([diagonal, offdiag, mass], axis=0).astype(jnp.float32)


def draw_right_side(key, part):
    key_base = jax.random.fold_in(key, 21)
    key_scale = jax.random.fold_in(key, 22)
    column = jnp.exp(jax.random.uniform(key_scale, (NX, NY, 1), jnp.float32, math.log(0.3), math.log(3.0)))
    ramp = 0.5 + jnp.arange(NY, dtype=jnp.float32)[None, :, None] / NY
    base = jnp.clip(jax.random.normal(key_base, (NX, NY, NZ), jnp.float32), -3.6, 3.6)
    return (base * column * ramp + 1.0).astype(jnp.float32)


def place_ends(array, stream_key, low, top_value):
    index_at = [jax.random.randint(jax.random.fold_in(stream_key, axis), (), 0, length) for axis, length in enumerate(array.shape)]
    widest = array.shape.index(max(array.shape))
    neighbour = index_at[:widest] + [(index_at[widest] + 1) % array.shape[widest]] + index_at[widest + 1:]
    return array.at[tuple(index_at)].set(low).at[tuple(neighbour)].set(top_value)


def setup_inputs(seed: int = 0) -> dict:
    arg_keys = jax.random.split(jax.random.key(seed), 4)
    labels = place_ends(jax.random.randint(arg_keys[0], (NX, NY, NZ), 0, LABELS), jax.random.fold_in(arg_keys[0], 1), 0, LABELS - 1).astype(jnp.int32)
    conductivity = draw_conductivity(jax.random.fold_in(arg_keys[3], 71), 0)
    right_side = draw_right_side(jax.random.fold_in(arg_keys[3], 71), 0)
    return {"labels": labels, "conductivity": conductivity, "right_side": right_side}


def neighbour_value(arr, shift_x, shift_y, shift_z, cell_grid):
    size_x, size_y, size_z = cell_grid
    return arr[..., 1 + shift_x:1 + shift_x + size_x, 1 + shift_y:1 + shift_y + size_y, 1 + shift_z:1 + shift_z + size_z]


def stencil_apply(padded_value, padded_sigma, self_coefficient):
    cell_grid = self_coefficient.shape
    value_entry = neighbour_value(padded_value, 0, 0, 0, cell_grid)
    total_flux = self_coefficient * value_entry
    for axis in range(3):
        for sign in (-1, 1):
            stencil_offset = [0, 0, 0]
            stencil_offset[axis] = sign
            face_flux = 0.5 * (neighbour_value(padded_sigma[axis], 0, 0, 0, cell_grid) + neighbour_value(padded_sigma[axis], stencil_offset[0], stencil_offset[1], stencil_offset[2], cell_grid))
            total_flux = total_flux + face_flux * (value_entry - neighbour_value(padded_value, stencil_offset[0], stencil_offset[1], stencil_offset[2], cell_grid))
    for first, second, comp in ((0, 1, 3), (0, 2, 4), (1, 2, 5)):
        for sign_a in (-1, 1):
            for sign_b in (-1, 1):
                stencil_offset = [0, 0, 0]
                stencil_offset[first] = sign_a
                stencil_offset[second] = sign_b
                cross_term = (0.25 * sign_a * sign_b) * (neighbour_value(padded_sigma[comp], 0, 0, 0, cell_grid) + neighbour_value(padded_sigma[comp], stencil_offset[0], stencil_offset[1], stencil_offset[2], cell_grid))
                total_flux = total_flux - cross_term * neighbour_value(padded_value, stencil_offset[0], stencil_offset[1], stencil_offset[2], cell_grid)
    return total_flux


def diagonal_of(padded_sigma, self_coefficient):
    cell_grid = self_coefficient.shape
    total_flux = self_coefficient
    for axis in range(3):
        for sign in (-1, 1):
            stencil_offset = [0, 0, 0]
            stencil_offset[axis] = sign
            total_flux = total_flux + 0.5 * (neighbour_value(padded_sigma[axis], 0, 0, 0, cell_grid) + neighbour_value(padded_sigma[axis], stencil_offset[0], stencil_offset[1], stencil_offset[2], cell_grid))
    return total_flux


def reference(labels, conductivity, right_side):
    extended = jnp.concatenate([jnp.zeros((7, 1), conductivity.dtype), conductivity], axis=1)
    label_pad = jnp.pad(labels.astype(jnp.int32) + 1, 1)
    planes = jnp.arange(labels.shape[0], dtype=jnp.int32)

    def slab_table(index):
        part = lax.dynamic_slice_in_dim(label_pad, index, 3, 0)
        table = jnp.take(extended, part, axis=1)
        return table[:6], table[6, 1:2, 1:-1, 1:-1]

    def diag_plane(index):
        padded_sigma, self_coefficient = slab_table(index)
        return diagonal_of(padded_sigma, self_coefficient)[0]

    diag = lax.map(diag_plane, planes)

    def operate(field):
        field_pad = jnp.pad(field, 1)

        def one_plane(index):
            padded_sigma, self_coefficient = slab_table(index)
            part = lax.dynamic_slice_in_dim(field_pad, index, 3, 0)
            return stencil_apply(part, padded_sigma, self_coefficient)[0]

        return lax.map(one_plane, planes)

    solution = jnp.zeros_like(right_side)
    residual = right_side
    precond = residual / diag
    direction = precond
    gamma = jnp.sum(residual * precond)
    for step in range(ITERS):
        image = operate(direction)
        alpha = gamma / jnp.sum(direction * image)
        solution = solution + alpha * direction
        residual = residual - alpha * image
        precond = residual / diag
        fresh = jnp.sum(residual * precond)
        direction = precond + (fresh / gamma) * direction
        gamma = fresh
    return solution
```

```python
import functools
import jax
import jax.numpy as jnp
from jax import lax
from jax.experimental import pallas as pl
from jax.experimental.pallas import tpu as pltpu
from jax.sharding import PartitionSpec as P

ITERS = 3
AXES = ("gx", "gy", "gz")
ROUNDS = ITERS + 1
MOMENTS = 2 * ITERS
LANES = 128
PAD = 8
CH = 16


def kernel(
    sizes, lab, cond, rhs, out, V, S, DI, PS, PR, ES, ER, HB, HS, PG, CP, MA, RS, RR,
    send_sem, recv_sem, ar_send, ar_recv,
):
    X, Y, Z = rhs.shape
    YE = Y + 2 * PAD
    TOP = PAD + Y
    me = [lax.axis_index(a) for a in AXES]
    f32 = jnp.float32

    directions = []
    for dx in (-1, 0, 1):
        for dy in (-1, 0, 1):
            for dz in (-1, 0, 1):
                d = (dx, dy, dz)
                live = sum(1 for t in d if t)
                if live in (1, 2) and all(n > 1 for t, n in zip(d, sizes) if t):
                    directions.append(d)

    def present(d):
        ok = None
        for t, m, n in zip(d, me, sizes):
            if t == 0:
                continue
            here = (m < n - 1) if t > 0 else (m > 0)
            ok = here if ok is None else jnp.logical_and(ok, here)
        return ok

    def places(d, r):
        dx, dy, dz = d
        rows_from = pl.ds(PAD, Y) if dy == 0 else (pl.ds(TOP - 8, 8) if dy > 0 else pl.ds(PAD, 8))
        rows_to = pl.ds(PAD, Y) if dy == 0 else (pl.ds(0, 8) if dy > 0 else pl.ds(TOP, 8))
        if dz == 0:
            if dx == 0:
                return V.at[r, pl.ds(1, X), rows_from], V.at[r, pl.ds(1, X), rows_to]
            fx, tx = (X, 0) if dx > 0 else (1, X + 1)
            return V.at[r, fx, rows_from], V.at[r, tx, rows_to]
        side = 0 if dz > 0 else 1
        if dx == 0:
            return PS.at[r, rows_from], PR.at[r, side, rows_to]
        slot = (0 if dx > 0 else 2) + side
        return ES.at[r], ER.at[r, slot]

    def copy(d, r):
        src, dst = places(d, r)
        m = directions.index(d)
        return pltpu.make_async_remote_copy(
            src_ref=src,
            dst_ref=dst,
            send_sem=send_sem.at[r, m],
            recv_sem=recv_sem.at[r, m],
            device_id=tuple(a + t for a, t in zip(me, d)),
            device_id_type=pl.DeviceIdType.MESH,
        )

    for d in [
        (dx, dy, dz)
        for dx in (-1, 0, 1)
        for dy in (-1, 0, 1)
        for dz in (-1, 0, 1)
        if sum(1 for t in (dx, dy, dz) if t) in (1, 2)
    ]:
        def clear(d=d):
            for r in range(ROUNDS):
                _, dst = places(d, r)
                dst[...] = jnp.zeros(dst.shape, f32)

        if d in directions:
            back = tuple(-t for t in d)
            pl.when(jnp.logical_not(present(back)))(clear)
        else:
            clear()

    def start(r):
        lane8 = lax.broadcasted_iota(jnp.int32, (8, LANES), 1)
        tile = jnp.zeros((8, LANES), f32)
        for col, at in enumerate((0, LANES - 1, 2 * (X - 1), 2 * (X - 1) - 1)):
            for k in range(Y // 8):
                to = col * (Y // 8) + k
                part = PS[r, pl.ds(PAD + 8 * k, 8), :]
                tile = jnp.where(lane8 == to, pltpu.roll(part, (to - at) % LANES, 1), tile)
        ES[r] = tile
        for d in directions:
            pl.when(present(d))(lambda d=d: copy(d, r).start())

    def wait(r):
        for d in directions:
            back = tuple(-t for t in d)
            pl.when(present(back))(lambda d=d: copy(d, r).wait_recv())

    lane_e = lax.broadcasted_iota(jnp.int32, (YE, LANES), 1)
    lane_c = lax.broadcasted_iota(jnp.int32, (CH, LANES), 1)
    lane_8 = lax.broadcasted_iota(jnp.int32, (8, LANES), 1)
    even = lane_e % 2 == 0
    lane_y = lax.broadcasted_iota(jnp.int32, (Y, LANES), 1)

    def build_halo(r):
        low = pltpu.roll(PR[r, 0], 1, 1)
        high = pltpu.roll(PR[r, 1], LANES - 1, 1)
        valid = jnp.logical_or(lane_e <= 2 * (X - 1), lane_e == LANES - 1)
        HB[...] = jnp.where(valid, jnp.where(even, low, high), 0.0)
        targets = (((LANES - 2), 3), ((LANES - 3), 2), (2 * X, 1), (2 * X - 1, 0))
        tiles = [ER[r, slot] for slot in range(4)]
        for k in range(Y // 8):
            rows = pl.ds(PAD + 8 * k, 8)
            part = HB[rows, :]
            for slot, (target, col) in enumerate(targets):
                at = col * (Y // 8) + k
                part = jnp.where(
                    lane_8 == target, pltpu.roll(tiles[slot], (target - at) % LANES, 1), part
                )
            HB[rows, :] = part

    def zm(a):
        return jnp.where(lane_c == 0, 0.0, pltpu.roll(a, 1, 1))

    def zp(a):
        return jnp.where(lane_c == LANES - 1, 0.0, pltpu.roll(a, LANES - 1, 1))

    def unpack(x, a):
        part = pltpu.roll(CP[pl.ds(a, CH), :], lax.rem(LANES - 2 * x, LANES), 1)
        return jnp.where(jnp.logical_or(lane_c == 0, lane_c == LANES - 1), part, 0.0)

    def pack(r, x, a, value):
        to = 2 * x
        other = lax.rem(2 * x + LANES - 1, LANES)
        mask = jnp.logical_or(lane_c == to, lane_c == other)
        rows = pl.ds(a, CH)
        PS[r, rows, :] = jnp.where(mask, pltpu.roll(value, to, 1), PS[r, rows, :])

    scale = (0.5, 0.5, 0.5, 0.25, 0.25, 0.25)
    count = cond.shape[1]
    table = [[cond[c, k] * scale[c] for k in range(count)] for c in range(6)]
    self_row = [cond[6, k] for k in range(count)]

    def lookup(values, components):
        outs = [jnp.zeros(values.shape, f32) for _ in components]
        for k in range(count):
            hit = values == f32(k + 1)
            outs = [
                jnp.where(hit, (self_row if c == 6 else table[c])[k], o)
                for c, o in zip(components, outs)
            ]
        return outs

    PS[...] = jnp.zeros(PS.shape, f32)
    MA[...] = jnp.zeros(MA.shape, f32)
    chunks = [PAD + i for i in range(0, Y, CH)]

    @pl.loop(0, X)
    def _(x):
        for a in chunks:
            value = (lab[x, pl.ds(a - PAD, CH), :] + 1).astype(f32)
            V[0, x + 1, pl.ds(a, CH), :] = value
            pack(0, x, a, value)

    start(0)
    wait(0)

    @pl.loop(0, X + 2)
    def _(x):
        for a in range(0, YE, CH):
            for c, s in enumerate(lookup(V[0, x, pl.ds(a, CH), :], range(6))):
                S[c, x, pl.ds(a, CH), :] = s

    build_halo(0)
    for i, s in enumerate(lookup(HB[...], (2, 4, 5))):
        HS[i] = s
    for i, s in enumerate(lookup(PS[0], (2, 4, 5))):
        PG[i] = s
    CP[...] = HS[0]

    def gather8(value):
        total = value[0:8]
        for i in range(8, CH, 8):
            total = total + value[i : i + 8]
        return total

    @pl.loop(0, X)
    def _(x):
        total = jnp.zeros((8, LANES), f32)
        for a in chunks:
            rows = pl.ds(a, CH)
            own = pl.ds(a - PAD, CH)
            (s6,) = lookup(V[0, x + 1, rows, :], (6,))
            s0, s1, s2 = (S[c, x + 1, rows, :] for c in range(3))
            diag = s6 + 2.0 * (s0 + s1 + s2)
            diag = diag + S[0, x, rows, :] + S[0, x + 2, rows, :]
            diag = diag + S[1, x + 1, pl.ds(a - 1, CH), :] + S[1, x + 1, pl.ds(a + 1, CH), :]
            diag = diag + zm(s2) + zp(s2) + unpack(x, a)
            inverse = 1.0 / diag
            DI[x, own, :] = inverse
            r0 = rhs[x, own, :]
            w = r0 * inverse
            V[1, x + 1, rows, :] = w
            pack(1, x, a, w)
            total = total + gather8(r0 * w)
        MA[0] = MA[0] + total

    for step in range(ITERS):
        r = step + 1
        start(r)
        wait(r)
        build_halo(r)
        sign = jnp.where(even, f32(-1.0), f32(1.0))

        def along_x(a):
            return pltpu.roll(a, LANES - 2, 1) - pltpu.roll(a, 2, 1)

        def along_y(a):
            return pltpu.roll(a, YE - 1, 0) - pltpu.roll(a, 1, 0)

        h = HB[...]
        CP[...] = (PG[0] + HS[0]) * h + sign * (
            PG[1] * along_x(h) + along_x(HS[1] * h) + PG[2] * along_y(h) + along_y(HS[2] * h)
        )
        last = step + 1 == ITERS

        @pl.loop(0, X)
        def _(x):
            odd = jnp.zeros((8, LANES), f32)
            evn = jnp.zeros((8, LANES), f32)
            for a in chunks:
                rows, up, down = pl.ds(a, CH), pl.ds(a + 1, CH), pl.ds(a - 1, CH)
                own = pl.ds(a - PAD, CH)
                v = V[r, x + 1, rows, :]
                vu, vd = V[r, x + 1, up, :], V[r, x + 1, down, :]
                p, pu, pd = V[r, x + 2, rows, :], V[r, x + 2, up, :], V[r, x + 2, down, :]
                m, mu, md = V[r, x, rows, :], V[r, x, up, :], V[r, x, down, :]
                dx = p - m
                dy = vu - vd
                q = S[0, x + 1, rows, :] * (m + p) + S[0, x, rows, :] * m + S[0, x + 2, rows, :] * p
                q = q + S[1, x + 1, rows, :] * (vu + vd)
                q = q + S[1, x + 1, up, :] * vu + S[1, x + 1, down, :] * vd
                q = q + S[3, x + 1, rows, :] * ((pu - pd) - (mu - md))
                q = q + (S[3, x + 2, up, :] * pu - S[3, x + 2, down, :] * pd)
                q = q - (S[3, x, up, :] * mu - S[3, x, down, :] * md)
                s2 = S[2, x + 1, rows, :]
                q = q + s2 * (zp(v) + zm(v))
                q = q + S[4, x + 1, rows, :] * (zp(dx) - zm(dx))
                q = q + S[5, x + 1, rows, :] * (zp(dy) - zm(dy))
                u = s2 * v
                g = S[4, x + 2, rows, :] * p - S[4, x, rows, :] * m
                g = g + S[5, x + 1, up, :] * vu - S[5, x + 1, down, :] * vd
                q = q + zp(u + g) + zm(u - g)
                q = q + unpack(x, a)
                odd = odd + gather8(v * q)
                if not last:
                    w = q * DI[x, own, :]
                    evn = evn + gather8(w * q)
                    V[r + 1, x + 1, rows, :] = w
                    pack(r + 1, x, a, w)
            MA[2 * step + 1] = MA[2 * step + 1] + odd
            if not last:
                MA[2 * step + 2] = MA[2 * step + 2] + evn

    row = lax.broadcasted_iota(jnp.int32, (8, LANES), 0)
    tile = jnp.zeros((8, LANES), f32)
    for k in range(MOMENTS):
        tile = jnp.where(row == k, jnp.sum(MA[k], axis=0, keepdims=True), tile)
    for order, i in enumerate((1, 2, 0)):
        n = sizes[i]
        if n == 1:
            continue
        RS[order] = tile
        copies = []
        for t in range(1, n):
            peer = list(me)
            peer[i] = lax.rem(me[i] + t, n)
            c = pltpu.make_async_remote_copy(
                src_ref=RS.at[order],
                dst_ref=RR.at[order, me[i]],
                send_sem=ar_send.at[order, t],
                recv_sem=ar_recv.at[order, t],
                device_id=tuple(peer),
                device_id_type=pl.DeviceIdType.MESH,
            )
            c.start()
            copies.append(c)
        RR[order, me[i]] = tile
        for c in copies:
            c.wait()
        tile = RR[order, 0]
        for t in range(1, n):
            tile = tile + RR[order, t]

    n0, n1, n2, n3, n4, n5 = (
        jnp.sum(tile[k : k + 1], axis=1, keepdims=True) for k in range(MOMENTS)
    )

    def inverse_of(d):
        return jnp.where(d > 0.0, 1.0 / d, 0.0)

    g00, g01, g02, g12, g22 = n0 - n1, n1 - n2, n2 - n3, n3 - n4, n4 - n5
    i0 = 1.0 / g00
    l1, l2 = g01 * i0, g02 * i0
    i1 = inverse_of(g02 - l1 * g01)
    e = g12 - l2 * g01
    l21 = e * i1
    i2 = inverse_of(g22 - l2 * g02 - l21 * e)
    y1 = n1 - l1 * n0
    y2 = n2 - l2 * n0 - l21 * y1
    c2 = y2 * i2
    c1 = y1 * i1 - l21 * c2
    c0 = n0 * i0 - l1 * c1 - l2 * c2

    @pl.loop(0, X)
    def _(x):
        for a in chunks:
            rows = pl.ds(a, CH)
            out[x, pl.ds(a - PAD, CH), :] = (
                c0 * V[1, x + 1, rows, :] + c1 * V[2, x + 1, rows, :] + c2 * V[3, x + 1, rows, :]
            )

    for r in range(ROUNDS):
        for d in directions:
            pl.when(present(d))(lambda d=d, r=r: copy(d, r).wait_send())


def solution(mesh):
    sizes = tuple(mesh.shape[a] for a in AXES)

    def local(labels, conductivity, right_side):
        X, Y, Z = right_side.shape
        YE = Y + 2 * PAD
        f32 = jnp.float32
        vmem = pltpu.VMEM
        return pl.pallas_call(
            functools.partial(kernel, sizes),
            out_shape=jax.ShapeDtypeStruct((X, Y, Z), f32),
            in_specs=[
                pl.BlockSpec(memory_space=pltpu.VMEM),
                pl.BlockSpec(memory_space=pltpu.SMEM),
                pl.BlockSpec(memory_space=pltpu.VMEM),
            ],
            out_specs=pl.BlockSpec(memory_space=pltpu.VMEM),
            scratch_shapes=[
                vmem((ROUNDS, X + 2, YE, Z), f32),
                vmem((6, X + 2, YE, Z), f32),
                vmem((X, Y, Z), f32),
                vmem((ROUNDS, YE, Z), f32),
                vmem((ROUNDS, 2, YE, Z), f32),
                vmem((ROUNDS, 8, Z), f32),
                vmem((ROUNDS, 4, 8, Z), f32),
                vmem((YE, Z), f32),
                vmem((3, YE, Z), f32),
                vmem((3, YE, Z), f32),
                vmem((YE, Z), f32),
                vmem((MOMENTS, 8, Z), f32),
                vmem((3, 8, Z), f32),
                vmem((3, max(sizes), 8, Z), f32),
                pltpu.SemaphoreType.DMA((ROUNDS, 18)),
                pltpu.SemaphoreType.DMA((ROUNDS, 18)),
                pltpu.SemaphoreType.DMA((3, max(sizes))),
                pltpu.SemaphoreType.DMA((3, max(sizes))),
            ],
            compiler_params=pltpu.CompilerParams(
                has_side_effects=True, vmem_limit_bytes=60 * 1024 * 1024
            ),
        )(labels, conductivity, right_side)

    return jax.shard_map(
        local,
        mesh=mesh,
        in_specs=(P("gx", "gy", "gz"), P(), P("gx", "gy", "gz")),
        out_specs=P("gx", "gy", "gz"),
        check_vma=False,
    )
```

```python
import functools
import itertools
import math
import jax
import jax.numpy as jnp
from jax import lax
from jax.experimental import pallas as pl
from jax.experimental.pallas import tpu as pltpu
from jax.sharding import PartitionSpec as P

ITERS = 3
AXES = ("gx", "gy", "gz")
ROUNDS = ITERS + 1
MOMENTS = 2 * ITERS
LANES = 128
PAD = 8
CH = 16


def kernel(
    sizes, lab_hbm, cond, rhs_hbm, out, lab, rhs, V0, V1, V2, V3, S, DI, PS, PR, ES, ER, HB, HS, PG, CP, MA, RS, RR,
    send_sem, recv_sem, ar_send, ar_recv, in_sem,
):
    V = (V0, V1, V2, V3)
    X, Y, Z = rhs.shape
    lab_copy = pltpu.make_async_copy(lab_hbm, lab, in_sem.at[0])
    lab_copy.start()
    rhs_copy = pltpu.make_async_copy(rhs_hbm, rhs, in_sem.at[1])
    rhs_copy.start()
    YE = Y + 2 * PAD
    TOP = PAD + Y
    me = [lax.axis_index(a) for a in AXES]
    f32 = jnp.float32

    directions = []
    for dx in (-1, 0, 1):
        for dy in (-1, 0, 1):
            for dz in (-1, 0, 1):
                d = (dx, dy, dz)
                live = sum(1 for t in d if t)
                if live in (1, 2) and all(n > 1 for t, n in zip(d, sizes) if t):
                    directions.append(d)

    def present(d):
        ok = None
        for t, m, n in zip(d, me, sizes):
            if t == 0:
                continue
            here = (m < n - 1) if t > 0 else (m > 0)
            ok = here if ok is None else jnp.logical_and(ok, here)
        return ok

    def places(d, r):
        dx, dy, dz = d
        rows_from = pl.ds(PAD, Y) if dy == 0 else (pl.ds(TOP - 8, 8) if dy > 0 else pl.ds(PAD, 8))
        rows_to = pl.ds(PAD, Y) if dy == 0 else (pl.ds(0, 8) if dy > 0 else pl.ds(TOP, 8))
        if dz == 0:
            if dx == 0:
                return V[r].at[pl.ds(1, X), rows_from], V[r].at[pl.ds(1, X), rows_to]
            fx, tx = (X, 0) if dx > 0 else (1, X + 1)
            return V[r].at[fx, rows_from], V[r].at[tx, rows_to]
        side = 0 if dz > 0 else 1
        if dx == 0:
            return PS.at[r, rows_from], PR.at[r, side, rows_to]
        slot = (0 if dx > 0 else 2) + side
        return ES.at[r], ER.at[r, slot]

    def copy(d, r):
        src, dst = places(d, r)
        m = directions.index(d)
        return pltpu.make_async_remote_copy(
            src_ref=src,
            dst_ref=dst,
            send_sem=send_sem.at[r, m],
            recv_sem=recv_sem.at[r, m],
            device_id=tuple(a + t for a, t in zip(me, d)),
            device_id_type=pl.DeviceIdType.MESH,
        )

    groups = [(0, 1, 2)] if math.prod(sizes) <= 32 else [(0, 1), (2,)]

    def offsets(group):
        ranges = [range(n) if i in group else (0,) for i, n in enumerate(sizes)]
        return [t for t in itertools.product(*ranges) if any(t)]

    def partner(t):
        return tuple(lax.rem(m + k, n) for m, k, n in zip(me, t, sizes))

    barrier = pltpu.get_barrier_semaphore()
    greeted = 0
    for group in groups:
        for t in offsets(group):
            pl.semaphore_signal(
                barrier, inc=1, device_id=partner(t), device_id_type=pl.DeviceIdType.MESH
            )
            greeted += 1
    if len(groups) > 1:
        for d in directions:
            pl.when(present(d))(
                lambda d=d: pl.semaphore_signal(
                    barrier,
                    inc=1,
                    device_id=tuple(a + t for a, t in zip(me, d)),
                    device_id_type=pl.DeviceIdType.MESH,
                )
            )
            greeted = greeted + jnp.where(present(d), 1, 0)

    for d in [
        (dx, dy, dz)
        for dx in (-1, 0, 1)
        for dy in (-1, 0, 1)
        for dz in (-1, 0, 1)
        if sum(1 for t in (dx, dy, dz) if t) in (1, 2)
    ]:
        def clear(d=d):
            for r in range(ROUNDS):
                _, dst = places(d, r)
                dst[...] = jnp.zeros(dst.shape, f32)

        if d in directions:
            back = tuple(-t for t in d)
            pl.when(jnp.logical_not(present(back)))(clear)
        else:
            clear()

    def start(r):
        lane8 = lax.broadcasted_iota(jnp.int32, (8, LANES), 1)
        tile = jnp.zeros((8, LANES), f32)
        for col, at in enumerate((0, LANES - 1, 2 * (X - 1), 2 * (X - 1) - 1)):
            for k in range(Y // 8):
                to = col * (Y // 8) + k
                part = PS[r, pl.ds(PAD + 8 * k, 8), :]
                tile = jnp.where(lane8 == to, pltpu.roll(part, (to - at) % LANES, 1), tile)
        ES[r] = tile
        for d in directions:
            pl.when(present(d))(lambda d=d: copy(d, r).start())

    def wait(r):
        for d in directions:
            back = tuple(-t for t in d)
            pl.when(present(back))(lambda d=d: copy(d, r).wait_recv())

    lane_e = lax.broadcasted_iota(jnp.int32, (YE, LANES), 1)
    lane_c = lax.broadcasted_iota(jnp.int32, (CH, LANES), 1)
    lane_8 = lax.broadcasted_iota(jnp.int32, (8, LANES), 1)
    even = lane_e % 2 == 0
    lane_y = lax.broadcasted_iota(jnp.int32, (Y, LANES), 1)

    def build_halo(r):
        low = pltpu.roll(PR[r, 0], 1, 1)
        high = pltpu.roll(PR[r, 1], LANES - 1, 1)
        valid = jnp.logical_or(lane_e <= 2 * (X - 1), lane_e == LANES - 1)
        HB[...] = jnp.where(valid, jnp.where(even, low, high), 0.0)
        targets = (((LANES - 2), 3), ((LANES - 3), 2), (2 * X, 1), (2 * X - 1, 0))
        tiles = [ER[r, slot] for slot in range(4)]
        for k in range(Y // 8):
            rows = pl.ds(PAD + 8 * k, 8)
            part = HB[rows, :]
            for slot, (target, col) in enumerate(targets):
                at = col * (Y // 8) + k
                part = jnp.where(
                    lane_8 == target, pltpu.roll(tiles[slot], (target - at) % LANES, 1), part
                )
            HB[rows, :] = part

    def zm(a):
        return jnp.where(lane_c == 0, 0.0, pltpu.roll(a, 1, 1))

    def zp(a):
        return jnp.where(lane_c == LANES - 1, 0.0, pltpu.roll(a, LANES - 1, 1))

    def unpack(x, a):
        part = pltpu.roll(CP[pl.ds(a, CH), :], lax.rem(LANES - 2 * x, LANES), 1)
        return jnp.where(jnp.logical_or(lane_c == 0, lane_c == LANES - 1), part, 0.0)

    def pack(r):
        @pl.loop(0, Y // 8)
        def _(k):
            rows = pl.ds(pl.multiple_of(PAD + 8 * k, 8), 8)
            parts = [V[r][x + 1, rows, :] for x in range(X)]
            width = 1
            while len(parts) > 1:
                joined = []
                for i in range(0, len(parts), 2):
                    low = parts[i]
                    if i + 1 < len(parts):
                        keep = jnp.logical_or(lane_8 <= 2 * width - 2, lane_8 == LANES - 1)
                        low = jnp.where(keep, low, pltpu.roll(parts[i + 1], 2 * width, 1))
                    joined.append(low)
                parts = joined
                width *= 2
            PS[r, rows, :] = parts[0]

    scale = (0.5, 0.5, 0.5, 0.25, 0.25, 0.25)
    count = cond.shape[1]
    table = [[cond[c, k] * scale[c] for k in range(count)] for c in range(6)]
    self_row = [cond[6, k] for k in range(count)]

    def lookup(values, components):
        outs = [jnp.zeros(values.shape, f32) for _ in components]
        for k in range(count):
            hit = values == f32(k + 1)
            outs = [
                jnp.where(hit, (self_row if c == 6 else table[c])[k], o)
                for c, o in zip(components, outs)
            ]
        return outs

    PS[...] = jnp.zeros(PS.shape, f32)
    lab_copy.wait()
    MA[...] = jnp.zeros(MA.shape, f32)
    chunks = [PAD + i for i in range(0, Y, CH)]

    @pl.loop(0, X)
    def _(x):
        for a in chunks:
            value = (lab[x, pl.ds(a - PAD, CH), :] + 1).astype(f32)
            V[0][x + 1, pl.ds(a, CH), :] = value

    pack(0)
    pl.semaphore_wait(barrier, greeted)
    start(0)
    wait(0)

    @pl.loop(0, X + 2, unroll=2)
    def _(x):
        for a in range(0, YE, CH):
            for c, s in enumerate(lookup(V[0][x, pl.ds(a, CH), :], range(6))):
                S[c, x, pl.ds(a, CH), :] = s

    build_halo(0)
    for i, s in enumerate(lookup(HB[...], (2, 4, 5))):
        HS[i] = s
    for i, s in enumerate(lookup(PS[0], (2, 4, 5))):
        PG[i] = s
    CP[...] = HS[0]
    rhs_copy.wait()

    def gather8(value):
        total = value[0:8]
        for i in range(8, CH, 8):
            total = total + value[i : i + 8]
        return total

    @pl.loop(0, X, unroll=2)
    def _(x):
        total = jnp.zeros((8, LANES), f32)
        for a in chunks:
            rows = pl.ds(a, CH)
            own = pl.ds(a - PAD, CH)
            (s6,) = lookup(V[0][x + 1, rows, :], (6,))
            s0, s1, s2 = (S[c, x + 1, rows, :] for c in range(3))
            diag = s6 + 2.0 * (s0 + s1 + s2)
            diag = diag + S[0, x, rows, :] + S[0, x + 2, rows, :]
            diag = diag + S[1, x + 1, pl.ds(a - 1, CH), :] + S[1, x + 1, pl.ds(a + 1, CH), :]
            diag = diag + zm(s2) + zp(s2) + unpack(x, a)
            inverse = 1.0 / diag
            DI[x, own, :] = inverse
            r0 = rhs[x, own, :]
            w = r0 * inverse
            V[1][x + 1, rows, :] = w
            total = total + gather8(r0 * w)
        MA[0] = MA[0] + total

    for step in range(ITERS):
        r = step + 1
        pack(r)
        start(r)
        wait(r)
        build_halo(r)
        sign = jnp.where(even, f32(-1.0), f32(1.0))

        def along_x(a):
            return pltpu.roll(a, LANES - 2, 1) - pltpu.roll(a, 2, 1)

        def along_y(a):
            return pltpu.roll(a, YE - 1, 0) - pltpu.roll(a, 1, 0)

        h = HB[...]
        CP[...] = (PG[0] + HS[0]) * h + sign * (
            PG[1] * along_x(h) + along_x(HS[1] * h) + PG[2] * along_y(h) + along_y(HS[2] * h)
        )
        last = step + 1 == ITERS

        @pl.loop(0, X, unroll=2)
        def _(x):
            odd = jnp.zeros((8, LANES), f32)
            evn = jnp.zeros((8, LANES), f32)
            for a in chunks:
                rows, up, down = pl.ds(a, CH), pl.ds(a + 1, CH), pl.ds(a - 1, CH)
                own = pl.ds(a - PAD, CH)
                v = V[r][x + 1, rows, :]
                vu, vd = V[r][x + 1, up, :], V[r][x + 1, down, :]
                p, pu, pd = V[r][x + 2, rows, :], V[r][x + 2, up, :], V[r][x + 2, down, :]
                m, mu, md = V[r][x, rows, :], V[r][x, up, :], V[r][x, down, :]
                dx = p - m
                dy = vu - vd
                q = S[0, x + 1, rows, :] * (m + p) + S[0, x, rows, :] * m + S[0, x + 2, rows, :] * p
                q = q + S[1, x + 1, rows, :] * (vu + vd)
                q = q + S[1, x + 1, up, :] * vu + S[1, x + 1, down, :] * vd
                q = q + S[3, x + 1, rows, :] * ((pu - pd) - (mu - md))
                q = q + (S[3, x + 2, up, :] * pu - S[3, x + 2, down, :] * pd)
                q = q - (S[3, x, up, :] * mu - S[3, x, down, :] * md)
                s2 = S[2, x + 1, rows, :]
                q = q + s2 * (zp(v) + zm(v))
                q = q + S[4, x + 1, rows, :] * (zp(dx) - zm(dx))
                q = q + S[5, x + 1, rows, :] * (zp(dy) - zm(dy))
                u = s2 * v
                g = S[4, x + 2, rows, :] * p - S[4, x, rows, :] * m
                g = g + S[5, x + 1, up, :] * vu - S[5, x + 1, down, :] * vd
                q = q + zp(u + g) + zm(u - g)
                q = q + unpack(x, a)
                odd = odd + gather8(v * q)
                if not last:
                    w = q * DI[x, own, :]
                    evn = evn + gather8(w * q)
                    V[r + 1][x + 1, rows, :] = w
            MA[2 * step + 1] = MA[2 * step + 1] + odd
            if not last:
                MA[2 * step + 2] = MA[2 * step + 2] + evn

    row = lax.broadcasted_iota(jnp.int32, (8, LANES), 0)
    tile = jnp.zeros((8, LANES), f32)
    for k in range(MOMENTS):
        tile = jnp.where(row == k, jnp.sum(MA[k], axis=0, keepdims=True), tile)
    for order, group in enumerate(groups):
        slot = 0
        members = 1
        for i in group:
            slot = slot * sizes[i] + me[i]
            members *= sizes[i]
        RS[order] = tile
        copies = []
        for index, t in enumerate(offsets(group)):
            c = pltpu.make_async_remote_copy(
                src_ref=RS.at[order],
                dst_ref=RR.at[order, slot],
                send_sem=ar_send.at[order, index],
                recv_sem=ar_recv.at[order, index],
                device_id=partner(t),
                device_id_type=pl.DeviceIdType.MESH,
            )
            c.start()
            copies.append(c)
        RR[order, slot] = tile
        for c in copies:
            c.wait()
        parts = [RR[order, t] for t in range(members)]
        while len(parts) > 1:
            parts = [sum(parts[i + 1 : i + 2], parts[i]) for i in range(0, len(parts), 2)]
        tile = parts[0]

    n0, n1, n2, n3, n4, n5 = (
        jnp.sum(tile[k : k + 1], axis=1, keepdims=True) for k in range(MOMENTS)
    )

    def inverse_of(d):
        return jnp.where(d > 0.0, 1.0 / d, 0.0)

    g00, g01, g02, g12, g22 = n0 - n1, n1 - n2, n2 - n3, n3 - n4, n4 - n5
    i0 = 1.0 / g00
    l1, l2 = g01 * i0, g02 * i0
    i1 = inverse_of(g02 - l1 * g01)
    e = g12 - l2 * g01
    l21 = e * i1
    i2 = inverse_of(g22 - l2 * g02 - l21 * e)
    y1 = n1 - l1 * n0
    y2 = n2 - l2 * n0 - l21 * y1
    c2 = y2 * i2
    c1 = y1 * i1 - l21 * c2
    c0 = n0 * i0 - l1 * c1 - l2 * c2

    @pl.loop(0, X)
    def _(x):
        for a in chunks:
            rows = pl.ds(a, CH)
            out[x, pl.ds(a - PAD, CH), :] = (
                c0 * V[1][x + 1, rows, :] + c1 * V[2][x + 1, rows, :] + c2 * V[3][x + 1, rows, :]
            )

    for r in range(ROUNDS):
        for d in directions:
            pl.when(present(d))(lambda d=d, r=r: copy(d, r).wait_send())


def solution(mesh):
    sizes = tuple(mesh.shape[a] for a in AXES)

    def local(labels, conductivity, right_side):
        X, Y, Z = right_side.shape
        YE = Y + 2 * PAD
        f32 = jnp.float32
        vmem = pltpu.VMEM
        return pl.pallas_call(
            functools.partial(kernel, sizes),
            out_shape=jax.ShapeDtypeStruct((X, Y, Z), f32),
            in_specs=[
                pl.BlockSpec(memory_space=pl.ANY),
                pl.BlockSpec(memory_space=pltpu.SMEM),
                pl.BlockSpec(memory_space=pl.ANY),
            ],
            out_specs=pl.BlockSpec(memory_space=pltpu.VMEM),
            scratch_shapes=[
                vmem((X, Y, Z), jnp.int32),
                vmem((X, Y, Z), f32),
                vmem((X + 2, YE, Z), f32),
                vmem((X + 2, YE, Z), f32),
                vmem((X + 2, YE, Z), f32),
                vmem((X + 2, YE, Z), f32),
                vmem((6, X + 2, YE, Z), f32),
                vmem((X, Y, Z), f32),
                vmem((ROUNDS, YE, Z), f32),
                vmem((ROUNDS, 2, YE, Z), f32),
                vmem((ROUNDS, 8, Z), f32),
                vmem((ROUNDS, 4, 8, Z), f32),
                vmem((YE, Z), f32),
                vmem((3, YE, Z), f32),
                vmem((3, YE, Z), f32),
                vmem((YE, Z), f32),
                vmem((MOMENTS, 8, Z), f32),
                vmem((2, 8, Z), f32),
                vmem((2, 32, 8, Z), f32),
                pltpu.SemaphoreType.DMA((ROUNDS, 18)),
                pltpu.SemaphoreType.DMA((ROUNDS, 18)),
                pltpu.SemaphoreType.DMA((2, 32)),
                pltpu.SemaphoreType.DMA((2, 32)),
                pltpu.SemaphoreType.DMA((2,)),
            ],
            compiler_params=pltpu.CompilerParams(
                collective_id=0, has_side_effects=True, vmem_limit_bytes=60 * 1024 * 1024
            ),
        )(labels, conductivity, right_side)

    return jax.shard_map(
        local,
        mesh=mesh,
        in_specs=(P("gx", "gy", "gz"), P(), P("gx", "gy", "gz")),
        out_specs=P("gx", "gy", "gz"),
        check_vma=False,
    )
```

```python
import functools
import itertools
import math
import jax
import jax.numpy as jnp
from jax import lax
from jax.experimental import pallas as pl
from jax.experimental.pallas import tpu as pltpu
from jax.sharding import PartitionSpec as P

ITERS = 3
AXES = ("gx", "gy", "gz")
ROUNDS = ITERS + 1
MOMENTS = 2 * ITERS
LANES = 128
PAD = 8
CH = 16


def kernel(
    sizes, lab_hbm, cond, rhs_hbm, out, lab, rhs, V0, V1, V2, V3, S, DI, PS, PR, ES, ER, HB, HS, PG, CP, MA, RS, RR,
    send_sem, recv_sem, ar_send, ar_recv, in_sem,
):
    V = (V0, V1, V2, V3)
    X, Y, Z = rhs.shape
    lab_copy = pltpu.make_async_copy(lab_hbm, lab, in_sem.at[0])
    lab_copy.start()
    rhs_copy = pltpu.make_async_copy(rhs_hbm, rhs, in_sem.at[1])
    rhs_copy.start()
    YE = Y + 2 * PAD
    TOP = PAD + Y
    me = [lax.axis_index(a) for a in AXES]
    f32 = jnp.float32

    directions = []
    for dx in (-1, 0, 1):
        for dy in (-1, 0, 1):
            for dz in (-1, 0, 1):
                d = (dx, dy, dz)
                live = sum(1 for t in d if t)
                if live in (1, 2) and all(n > 1 for t, n in zip(d, sizes) if t):
                    directions.append(d)

    def present(d):
        ok = None
        for t, m, n in zip(d, me, sizes):
            if t == 0:
                continue
            here = (m < n - 1) if t > 0 else (m > 0)
            ok = here if ok is None else jnp.logical_and(ok, here)
        return ok

    def places(d, r):
        dx, dy, dz = d
        rows_from = pl.ds(PAD, Y) if dy == 0 else (pl.ds(TOP - 8, 8) if dy > 0 else pl.ds(PAD, 8))
        rows_to = pl.ds(PAD, Y) if dy == 0 else (pl.ds(0, 8) if dy > 0 else pl.ds(TOP, 8))
        if dz == 0:
            if dx == 0:
                return V[r].at[pl.ds(1, X), rows_from], V[r].at[pl.ds(1, X), rows_to]
            fx, tx = (X, 0) if dx > 0 else (1, X + 1)
            return V[r].at[fx, rows_from], V[r].at[tx, rows_to]
        side = 0 if dz > 0 else 1
        if dx == 0:
            return PS.at[r, rows_from], PR.at[r, side, rows_to]
        slot = (0 if dx > 0 else 2) + side
        return ES.at[r], ER.at[r, slot]

    def copy(d, r):
        src, dst = places(d, r)
        m = directions.index(d)
        return pltpu.make_async_remote_copy(
            src_ref=src,
            dst_ref=dst,
            send_sem=send_sem.at[r, m],
            recv_sem=recv_sem.at[r, m],
            device_id=tuple(a + t for a, t in zip(me, d)),
            device_id_type=pl.DeviceIdType.MESH,
        )

    groups = [(0, 1, 2)] if math.prod(sizes) <= 32 else [(0, 1), (2,)]

    def offsets(group):
        ranges = [range(n) if i in group else (0,) for i, n in enumerate(sizes)]
        return [t for t in itertools.product(*ranges) if any(t)]

    def partner(t):
        return tuple(lax.rem(m + k, n) for m, k, n in zip(me, t, sizes))

    barrier = pltpu.get_barrier_semaphore()
    greeted = 0
    for group in groups:
        for t in offsets(group):
            pl.semaphore_signal(
                barrier, inc=1, device_id=partner(t), device_id_type=pl.DeviceIdType.MESH
            )
            greeted += 1
    if len(groups) > 1:
        for d in directions:
            pl.when(present(d))(
                lambda d=d: pl.semaphore_signal(
                    barrier,
                    inc=1,
                    device_id=tuple(a + t for a, t in zip(me, d)),
                    device_id_type=pl.DeviceIdType.MESH,
                )
            )
            greeted = greeted + jnp.where(present(d), 1, 0)

    for d in [
        (dx, dy, dz)
        for dx in (-1, 0, 1)
        for dy in (-1, 0, 1)
        for dz in (-1, 0, 1)
        if sum(1 for t in (dx, dy, dz) if t) in (1, 2)
    ]:
        def clear(d=d):
            for r in range(ROUNDS):
                _, dst = places(d, r)
                dst[...] = jnp.zeros(dst.shape, f32)

        if d in directions:
            back = tuple(-t for t in d)
            pl.when(jnp.logical_not(present(back)))(clear)
        else:
            clear()

    def start(r):
        lane8 = lax.broadcasted_iota(jnp.int32, (8, LANES), 1)
        tile = jnp.zeros((8, LANES), f32)
        for col, at in enumerate((0, LANES - 1, 2 * (X - 1), 2 * (X - 1) - 1)):
            for k in range(Y // 8):
                to = col * (Y // 8) + k
                part = PS[r, pl.ds(PAD + 8 * k, 8), :]
                tile = jnp.where(lane8 == to, pltpu.roll(part, (to - at) % LANES, 1), tile)
        ES[r] = tile
        for d in directions:
            pl.when(present(d))(lambda d=d: copy(d, r).start())

    def wait(r):
        for d in directions:
            back = tuple(-t for t in d)
            pl.when(present(back))(lambda d=d: copy(d, r).wait_recv())

    lane_e = lax.broadcasted_iota(jnp.int32, (YE, LANES), 1)
    lane_c = lax.broadcasted_iota(jnp.int32, (CH, LANES), 1)
    lane_8 = lax.broadcasted_iota(jnp.int32, (8, LANES), 1)
    even = lane_e % 2 == 0
    lane_y = lax.broadcasted_iota(jnp.int32, (Y, LANES), 1)

    def build_halo(r):
        low = pltpu.roll(PR[r, 0], 1, 1)
        high = pltpu.roll(PR[r, 1], LANES - 1, 1)
        valid = jnp.logical_or(lane_e <= 2 * (X - 1), lane_e == LANES - 1)
        HB[...] = jnp.where(valid, jnp.where(even, low, high), 0.0)
        targets = (((LANES - 2), 3), ((LANES - 3), 2), (2 * X, 1), (2 * X - 1, 0))
        tiles = [ER[r, slot] for slot in range(4)]
        for k in range(Y // 8):
            rows = pl.ds(PAD + 8 * k, 8)
            part = HB[rows, :]
            for slot, (target, col) in enumerate(targets):
                at = col * (Y // 8) + k
                part = jnp.where(
                    lane_8 == target, pltpu.roll(tiles[slot], (target - at) % LANES, 1), part
                )
            HB[rows, :] = part

    def zm(a):
        return jnp.where(lane_c == 0, 0.0, pltpu.roll(a, 1, 1))

    def zp(a):
        return jnp.where(lane_c == LANES - 1, 0.0, pltpu.roll(a, LANES - 1, 1))

    def unpack(x, a):
        part = pltpu.roll(CP[pl.ds(a, CH), :], lax.rem(LANES - 2 * x, LANES), 1)
        return jnp.where(jnp.logical_or(lane_c == 0, lane_c == LANES - 1), part, 0.0)

    def pack(r):
        @pl.loop(0, Y // 8, unroll=4)
        def _(k):
            rows = pl.ds(pl.multiple_of(PAD + 8 * k, 8), 8)
            parts = [V[r][x + 1, rows, :] for x in range(X)]
            width = 1
            while len(parts) > 1:
                joined = []
                for i in range(0, len(parts), 2):
                    low = parts[i]
                    if i + 1 < len(parts):
                        keep = jnp.logical_or(lane_8 <= 2 * width - 2, lane_8 == LANES - 1)
                        low = jnp.where(keep, low, pltpu.roll(parts[i + 1], 2 * width, 1))
                    joined.append(low)
                parts = joined
                width *= 2
            PS[r, rows, :] = parts[0]

    scale = (0.5, 0.5, 0.5, 0.25, 0.25, 0.25)
    count = cond.shape[1]
    table = [[cond[c, k] * scale[c] for k in range(count)] for c in range(6)]
    self_row = [cond[6, k] for k in range(count)]

    def lookup(values, components):
        outs = [jnp.zeros(values.shape, f32) for _ in components]
        for k in range(count):
            hit = values == f32(k + 1)
            outs = [
                jnp.where(hit, (self_row if c == 6 else table[c])[k], o)
                for c, o in zip(components, outs)
            ]
        return outs

    PS[...] = jnp.zeros(PS.shape, f32)
    lab_copy.wait()
    MA[...] = jnp.zeros(MA.shape, f32)
    chunks = [PAD + i for i in range(0, Y, CH)]

    @pl.loop(0, X)
    def _(x):
        for a in chunks:
            value = (lab[x, pl.ds(a - PAD, CH), :] + 1).astype(f32)
            V[0][x + 1, pl.ds(a, CH), :] = value

    pack(0)
    pl.semaphore_wait(barrier, greeted)
    start(0)
    wait(0)

    @pl.loop(0, X + 2, unroll=2)
    def _(x):
        for a in range(0, YE, CH):
            for c, s in enumerate(lookup(V[0][x, pl.ds(a, CH), :], range(6))):
                S[c, x, pl.ds(a, CH), :] = s

    build_halo(0)
    for i, s in enumerate(lookup(HB[...], (2, 4, 5))):
        HS[i] = s
    for i, s in enumerate(lookup(PS[0], (2, 4, 5))):
        PG[i] = s
    CP[...] = HS[0]
    rhs_copy.wait()

    def gather8(value):
        total = value[0:8]
        for i in range(8, CH, 8):
            total = total + value[i : i + 8]
        return total

    @pl.loop(0, X, unroll=4)
    def _(x):
        total = jnp.zeros((8, LANES), f32)
        for a in chunks:
            rows = pl.ds(a, CH)
            own = pl.ds(a - PAD, CH)
            (s6,) = lookup(V[0][x + 1, rows, :], (6,))
            s0, s1, s2 = (S[c, x + 1, rows, :] for c in range(3))
            diag = s6 + 2.0 * (s0 + s1 + s2)
            diag = diag + S[0, x, rows, :] + S[0, x + 2, rows, :]
            diag = diag + S[1, x + 1, pl.ds(a - 1, CH), :] + S[1, x + 1, pl.ds(a + 1, CH), :]
            diag = diag + zm(s2) + zp(s2) + unpack(x, a)
            inverse = 1.0 / diag
            DI[x, own, :] = inverse
            r0 = rhs[x, own, :]
            w = r0 * inverse
            V[1][x + 1, rows, :] = w
            total = total + gather8(r0 * w)
        MA[0] = MA[0] + total

    for step in range(ITERS):
        r = step + 1
        pack(r)
        start(r)
        wait(r)
        build_halo(r)
        sign = jnp.where(even, f32(-1.0), f32(1.0))

        def along_x(a):
            return pltpu.roll(a, LANES - 2, 1) - pltpu.roll(a, 2, 1)

        def along_y(a):
            return pltpu.roll(a, YE - 1, 0) - pltpu.roll(a, 1, 0)

        h = HB[...]
        CP[...] = (PG[0] + HS[0]) * h + sign * (
            PG[1] * along_x(h) + along_x(HS[1] * h) + PG[2] * along_y(h) + along_y(HS[2] * h)
        )
        last = step + 1 == ITERS

        @pl.loop(0, X, unroll=4)
        def _(x):
            odd = jnp.zeros((8, LANES), f32)
            evn = jnp.zeros((8, LANES), f32)
            for a in chunks:
                rows, up, down = pl.ds(a, CH), pl.ds(a + 1, CH), pl.ds(a - 1, CH)
                own = pl.ds(a - PAD, CH)
                v = V[r][x + 1, rows, :]
                vu, vd = V[r][x + 1, up, :], V[r][x + 1, down, :]
                p, pu, pd = V[r][x + 2, rows, :], V[r][x + 2, up, :], V[r][x + 2, down, :]
                m, mu, md = V[r][x, rows, :], V[r][x, up, :], V[r][x, down, :]
                dx = p - m
                dy = vu - vd
                q = S[0, x + 1, rows, :] * (m + p) + S[0, x, rows, :] * m + S[0, x + 2, rows, :] * p
                q = q + S[1, x + 1, rows, :] * (vu + vd)
                q = q + S[1, x + 1, up, :] * vu + S[1, x + 1, down, :] * vd
                q = q + S[3, x + 1, rows, :] * ((pu - pd) - (mu - md))
                q = q + (S[3, x + 2, up, :] * pu - S[3, x + 2, down, :] * pd)
                q = q - (S[3, x, up, :] * mu - S[3, x, down, :] * md)
                s2 = S[2, x + 1, rows, :]
                q = q + s2 * (zp(v) + zm(v))
                q = q + S[4, x + 1, rows, :] * (zp(dx) - zm(dx))
                q = q + S[5, x + 1, rows, :] * (zp(dy) - zm(dy))
                u = s2 * v
                g = S[4, x + 2, rows, :] * p - S[4, x, rows, :] * m
                g = g + S[5, x + 1, up, :] * vu - S[5, x + 1, down, :] * vd
                q = q + zp(u + g) + zm(u - g)
                q = q + unpack(x, a)
                odd = odd + gather8(v * q)
                if not last:
                    w = q * DI[x, own, :]
                    evn = evn + gather8(w * q)
                    V[r + 1][x + 1, rows, :] = w
            MA[2 * step + 1] = MA[2 * step + 1] + odd
            if not last:
                MA[2 * step + 2] = MA[2 * step + 2] + evn

    row = lax.broadcasted_iota(jnp.int32, (8, LANES), 0)
    tile = jnp.zeros((8, LANES), f32)
    for k in range(MOMENTS):
        tile = jnp.where(row == k, jnp.sum(MA[k], axis=0, keepdims=True), tile)
    for order, group in enumerate(groups):
        slot = 0
        members = 1
        for i in group:
            slot = slot * sizes[i] + me[i]
            members *= sizes[i]
        RS[order] = tile
        copies = []
        for index, t in enumerate(offsets(group)):
            c = pltpu.make_async_remote_copy(
                src_ref=RS.at[order],
                dst_ref=RR.at[order, slot],
                send_sem=ar_send.at[order, index],
                recv_sem=ar_recv.at[order, index],
                device_id=partner(t),
                device_id_type=pl.DeviceIdType.MESH,
            )
            c.start()
            copies.append(c)
        RR[order, slot] = tile
        for c in copies:
            c.wait()
        parts = [RR[order, t] for t in range(members)]
        while len(parts) > 1:
            parts = [sum(parts[i + 1 : i + 2], parts[i]) for i in range(0, len(parts), 2)]
        tile = parts[0]

    n0, n1, n2, n3, n4, n5 = (
        jnp.sum(tile[k : k + 1], axis=1, keepdims=True) for k in range(MOMENTS)
    )

    def inverse_of(d):
        return jnp.where(d > 0.0, 1.0 / d, 0.0)

    g00, g01, g02, g12, g22 = n0 - n1, n1 - n2, n2 - n3, n3 - n4, n4 - n5
    i0 = 1.0 / g00
    l1, l2 = g01 * i0, g02 * i0
    i1 = inverse_of(g02 - l1 * g01)
    e = g12 - l2 * g01
    l21 = e * i1
    i2 = inverse_of(g22 - l2 * g02 - l21 * e)
    y1 = n1 - l1 * n0
    y2 = n2 - l2 * n0 - l21 * y1
    c2 = y2 * i2
    c1 = y1 * i1 - l21 * c2
    c0 = n0 * i0 - l1 * c1 - l2 * c2

    @pl.loop(0, X)
    def _(x):
        for a in chunks:
            rows = pl.ds(a, CH)
            out[x, pl.ds(a - PAD, CH), :] = (
                c0 * V[1][x + 1, rows, :] + c1 * V[2][x + 1, rows, :] + c2 * V[3][x + 1, rows, :]
            )

    for r in range(ROUNDS):
        for d in directions:
            pl.when(present(d))(lambda d=d, r=r: copy(d, r).wait_send())


def solution(mesh):
    sizes = tuple(mesh.shape[a] for a in AXES)

    def local(labels, conductivity, right_side):
        X, Y, Z = right_side.shape
        YE = Y + 2 * PAD
        f32 = jnp.float32
        vmem = pltpu.VMEM
        return pl.pallas_call(
            functools.partial(kernel, sizes),
            out_shape=jax.ShapeDtypeStruct((X, Y, Z), f32),
            in_specs=[
                pl.BlockSpec(memory_space=pl.ANY),
                pl.BlockSpec(memory_space=pltpu.SMEM),
                pl.BlockSpec(memory_space=pl.ANY),
            ],
            out_specs=pl.BlockSpec(memory_space=pltpu.VMEM),
            scratch_shapes=[
                vmem((X, Y, Z), jnp.int32),
                vmem((X, Y, Z), f32),
                vmem((X + 2, YE, Z), f32),
                vmem((X + 2, YE, Z), f32),
                vmem((X + 2, YE, Z), f32),
                vmem((X + 2, YE, Z), f32),
                vmem((6, X + 2, YE, Z), f32),
                vmem((X, Y, Z), f32),
                vmem((ROUNDS, YE, Z), f32),
                vmem((ROUNDS, 2, YE, Z), f32),
                vmem((ROUNDS, 8, Z), f32),
                vmem((ROUNDS, 4, 8, Z), f32),
                vmem((YE, Z), f32),
                vmem((3, YE, Z), f32),
                vmem((3, YE, Z), f32),
                vmem((YE, Z), f32),
                vmem((MOMENTS, 8, Z), f32),
                vmem((2, 8, Z), f32),
                vmem((2, 32, 8, Z), f32),
                pltpu.SemaphoreType.DMA((ROUNDS, 18)),
                pltpu.SemaphoreType.DMA((ROUNDS, 18)),
                pltpu.SemaphoreType.DMA((2, 32)),
                pltpu.SemaphoreType.DMA((2, 32)),
                pltpu.SemaphoreType.DMA((2,)),
            ],
            compiler_params=pltpu.CompilerParams(
                collective_id=0, has_side_effects=True, vmem_limit_bytes=60 * 1024 * 1024
            ),
        )(labels, conductivity, right_side)

    return jax.shard_map(
        local,
        mesh=mesh,
        in_specs=(P("gx", "gy", "gz"), P(), P("gx", "gy", "gz")),
        out_specs=P("gx", "gy", "gz"),
        check_vma=False,
    )
```
